32 devices in a mesh: gx: 32 (over z, y, x, core).
Axes of the slice: x: 2, y: 2, z: 4, core: 2. Of those that a mesh axis runs over, the one named last changes fastest.
Arguments:
- nodal_values: float32 [128, 512, 256], P('gx'), may hold values from -6 to 6
Outputs:
- surpluses: float32 [128, 512, 256], P('gx')
The draws below stay inside these ranges and needn't reach their ends.
All inputs are finite; a program needn't handle non-finite values.
Results may differ from the reference program's by a relative error of at most 0.00005.
Values sent between devices are 32-bit elements; how exact they have to be, the bound alone decides.
No kernel may reach another device: no remote copies, remote signals or barrier semaphores. Data moves between devices by JAX's collectives and lax.ppermute only.
A program may use at most 64 MiB of HBM per device.

```python
import jax
import jax.numpy as jnp
from jax import lax

NY = 512
NZ = 256
PLANES = 4
NX = 128


def block_levels(own_key, dims, pieces, smallest, top_value):
    factor_of, own = 1.0, jax.random.fold_in(own_key, 6)
    for position, blocks in pieces:
        draws = jnp.exp(jax.random.uniform(jax.random.fold_in(own, position), (blocks,), jnp.float32, smallest / len(pieces), top_value / len(pieces)))
        factor_of = factor_of * jnp.repeat(draws, dims[position] // blocks).reshape([-1 if axis == position else 1 for axis in range(len(dims))])
    return factor_of


def centred(key, dims, spread, limit, cuts=(), held_as=jnp.bfloat16):
    array = spread * jax.random.normal(key, dims, jnp.float32)
    if cuts:
        array = array * block_levels(key, dims, cuts, -0.22, 0.18)
    return jnp.clip(array, -limit, limit).astype(held_as)


def setup_inputs(seed: int = 0) -> dict:
    key_list = jax.random.split(jax.random.key(seed), 2)
    return {
        "nodal_values": centred(key_list[0], (NX, NY, NZ), 1.0, 6.0, ((0, 32),), jnp.float32),
    }


def lift_axis(values, strides):
    result = values
    for stride in strides:
        parents = values[0::2 * stride]
        children = values[stride::2 * stride]
        updated = children - 0.5 * (parents + jnp.roll(parents, -1, axis=0))
        result = result.at[stride::2 * stride].set(updated)
    return result


def all_strides(length):
    return [2 ** exponent for exponent in range(int(length).bit_length() - 1)]


def lift_planes(blocks):
    second = jnp.moveaxis(lift_axis(jnp.moveaxis(blocks, 1, 0), all_strides(NY)), 0, 1)
    return jnp.moveaxis(lift_axis(jnp.moveaxis(second, 2, 0), all_strides(NZ)), 0, 2)


def reference(nodal_values):
    anchor = 2 * PLANES - 1
    shifted = jnp.roll(nodal_values, -anchor, axis=0)
    across = jnp.roll(lift_axis(shifted, all_strides(NX)), anchor, axis=0)
    blocks = across.reshape(NX // 16, 16, NY, NZ)
    return lax.map(lift_planes, blocks).reshape(NX, NY, NZ)
```

```python
import jax
import jax.numpy as jnp
from jax import lax
from jax.experimental import pallas as pl
from jax.experimental.pallas import tpu as pltpu
from jax.sharding import PartitionSpec as P


def strides_of(length):
    return [2**exponent for exponent in range(length.bit_length() - 1)]


def lowest_bit(index):
    return index & -index


def lift_rows(plane):
    length = plane.shape[0]
    row = lax.broadcasted_iota(jnp.int32, (length, 128), 0)
    row = jnp.concatenate([row] * (plane.shape[1] // 128), axis=1)
    parents = jnp.zeros_like(plane)
    for stride in strides_of(length):
        both = pltpu.roll(plane, stride, 0) + pltpu.roll(plane, length - stride, 0)
        parents = jnp.where((row & (2 * stride - 1)) == stride, both, parents)
    return plane - 0.5 * parents


def parent_counts(length):
    parent = lax.broadcasted_iota(jnp.int32, (length, length), 0)
    child = lax.broadcasted_iota(jnp.int32, (length, length), 1)
    step = child & -child
    low = ((child - step) == parent) & (child > 0)
    high = (((child + step) & (length - 1)) == parent) & (child > 0)
    return (low.astype(jnp.float32) + high.astype(jnp.float32)).astype(jnp.bfloat16)


def lift_columns(plane, counts):
    upper = plane.astype(jnp.bfloat16)
    rest = (plane - upper.astype(jnp.float32)).astype(jnp.bfloat16)
    parents = jnp.dot(upper, counts, preferred_element_type=jnp.float32)
    parents += jnp.dot(rest, counts, preferred_element_type=jnp.float32)
    return plane - 0.5 * parents


def lift_plane(plane):
    return lift_columns(lift_rows(plane), parent_counts(plane.shape[1]))


def head_kernel(x_ref, o_ref):
    o_ref[0] = lift_plane(x_ref[0])


def lift_head(values):
    planes, rows, columns = values.shape
    return pl.pallas_call(
        head_kernel,
        grid=(1,),
        in_specs=[pl.BlockSpec((1, rows, columns), lambda i: (planes - 1, 0, 0))],
        out_specs=pl.BlockSpec((1, rows, columns), lambda i: (0, 0, 0)),
        out_shape=jax.ShapeDtypeStruct((1, rows, columns), jnp.float32),
        name="lift_head",
    )(values)


def local_kernel(x_ref, head_ref, o_ref):
    head = head_ref[0]
    middle = lift_plane(x_ref[1])
    o_ref[0] = lift_plane(x_ref[0]) - 0.5 * middle
    o_ref[1] = middle - 0.5 * head
    o_ref[2] = lift_plane(x_ref[2]) - 0.5 * (middle + head)


def lift_local(values, head):
    planes, rows, columns = values.shape
    return pl.pallas_call(
        local_kernel,
        grid=(1,),
        in_specs=[
            pl.BlockSpec((planes, rows, columns), lambda i: (0, 0, 0)),
            pl.BlockSpec((1, rows, columns), lambda i: (0, 0, 0)),
        ],
        out_specs=pl.BlockSpec((planes - 1, rows, columns), lambda i: (0, 0, 0)),
        out_shape=jax.ShapeDtypeStruct((planes - 1, rows, columns), jnp.float32),
        name="lift_local",
    )(values, head)


def finish_kernel(part_ref, head_ref, lower_ref, *refs):
    received, o_ref = refs[:-1], refs[-1]
    lower = 0.5 * lower_ref[0]
    coarse = received[0][0]
    for ref in received[1:]:
        coarse = coarse + ref[0]
    o_ref[0] = part_ref[0] - lower
    o_ref[1] = part_ref[1] - lower
    o_ref[2] = part_ref[2]
    o_ref[3] = head_ref[0] - 0.5 * coarse


def finish(partial, head, lower, received):
    count, rows, columns = partial.shape
    chunk = rows // 4
    one = pl.BlockSpec((1, chunk, columns), lambda i: (0, i, 0))
    return pl.pallas_call(
        finish_kernel,
        grid=(rows // chunk,),
        in_specs=[pl.BlockSpec((count, chunk, columns), lambda i: (0, i, 0))]
        + [one] * (2 + len(received)),
        out_specs=pl.BlockSpec((count + 1, chunk, columns), lambda i: (0, i, 0)),
        out_shape=jax.ShapeDtypeStruct((count + 1, rows, columns), jnp.float32),
        name="finish",
    )(partial, head, lower, *received)


def on_device(nodal_values):
    size = lax.axis_size("gx")
    coarse_index = jnp.mod(lax.axis_index("gx") - 1, size)
    head = lift_head(nodal_values)

    def route(distance, children):
        return [((c + distance + 1) % size, (c + 1) % size) for c in children]

    lower = lax.ppermute(head, "gx", route(-1, range(size)))
    received = []
    for stride in reversed(strides_of(size)):
        children = [c for c in range(1, size) if lowest_bit(c) == stride]
        if stride > 1:
            low = lax.ppermute(head, "gx", route(-stride, children))
            received.append(low)
        if 2 * stride < size:
            received.append(lax.ppermute(head, "gx", route(stride, children)))
    top = received[0]
    received[0] = top + top
    received.append(jnp.where((coarse_index & 1) == 1, lower, 0.0))
    return finish(lift_local(nodal_values, head), head, lower, received)


def solution(mesh):
    in_specs = (P("gx", None, None),)
    out_specs = P("gx", None, None)
    return jax.shard_map(
        on_device, mesh=mesh, in_specs=in_specs, out_specs=out_specs, check_vma=False
    )
```

```python
import jax
import jax.numpy as jnp
from jax import lax
from jax.experimental import pallas as pl
from jax.experimental.pallas import tpu as pltpu
from jax.sharding import PartitionSpec as P


def strides_of(length):
    return [2**exponent for exponent in range(length.bit_length() - 1)]


def lift_rows(plane):
    length = plane.shape[0]
    row = lax.broadcasted_iota(jnp.int32, (length, 128), 0)
    row = jnp.concatenate([row] * (plane.shape[1] // 128), axis=1)
    parents = jnp.zeros_like(plane)
    for stride in strides_of(length):
        both = pltpu.roll(plane, stride, 0) + pltpu.roll(plane, length - stride, 0)
        parents = jnp.where((row & (2 * stride - 1)) == stride, both, parents)
    return plane - 0.5 * parents


def parent_counts(length):
    parent = lax.broadcasted_iota(jnp.int32, (length, length), 0)
    child = lax.broadcasted_iota(jnp.int32, (length, length), 1)
    step = child & -child
    low = ((child - step) == parent) & (child > 0)
    high = (((child + step) & (length - 1)) == parent) & (child > 0)
    return (low.astype(jnp.float32) + high.astype(jnp.float32)).astype(jnp.bfloat16)


def lift_columns(plane, counts):
    upper = plane.astype(jnp.bfloat16)
    rest = (plane - upper.astype(jnp.float32)).astype(jnp.bfloat16)
    parents = jnp.dot(upper, counts, preferred_element_type=jnp.float32)
    parents += jnp.dot(rest, counts, preferred_element_type=jnp.float32)
    return plane - 0.5 * parents


def lift_plane(plane):
    return lift_columns(lift_rows(plane), parent_counts(plane.shape[1]))


def head_kernel(x_ref, o_ref):
    o_ref[0] = lift_plane(x_ref[0])


def lift_head(values):
    planes, rows, columns = values.shape
    return pl.pallas_call(
        head_kernel,
        grid=(1,),
        in_specs=[pl.BlockSpec((1, rows, columns), lambda i: (planes - 1, 0, 0))],
        out_specs=pl.BlockSpec((1, rows, columns), lambda i: (0, 0, 0)),
        out_shape=jax.ShapeDtypeStruct((1, rows, columns), jnp.float32),
        name="lift_head",
    )(values)


def local_kernel(x_ref, head_ref, lower_ref, o_ref):
    head = head_ref[0]
    lower = 0.5 * lower_ref[0]
    middle = lift_plane(x_ref[1])
    o_ref[0] = lift_plane(x_ref[0]) - 0.5 * middle - lower
    o_ref[1] = middle - 0.5 * head - lower
    o_ref[2] = lift_plane(x_ref[2]) - 0.5 * (middle + head)


def lift_local(values, head, lower):
    planes, rows, columns = values.shape
    one = pl.BlockSpec((1, rows, columns), lambda i: (0, 0, 0))
    most = pl.BlockSpec((planes - 1, rows, columns), lambda i: (0, 0, 0))
    return pl.pallas_call(
        local_kernel,
        grid=(1,),
        in_specs=[most, one, one],
        out_specs=most,
        out_shape=jax.ShapeDtypeStruct(values.shape, jnp.float32),
        name="lift_local",
    )(values, head, lower)


CHUNKS = 4


def last_kernel(case_ref, out_in_ref, head_ref, *refs, cases):
    del out_in_ref
    arrays, (o_ref, own, low, high, result, sems, out_sems) = refs[:-7], refs[-7:]
    last = o_ref.shape[0] - 1
    rows = o_ref.shape[1]
    parts = [pl.ds(i * (rows // CHUNKS), rows // CHUNKS) for i in range(CHUNKS)]
    case = case_ref[0]

    def fetch(source, target, k, i):
        return pltpu.make_async_copy(
            source.at[0, parts[i]], target.at[parts[i]], sems.at[k, i]
        )

    for i in range(CHUNKS):
        fetch(head_ref, own, 0, i).start()
    for number, (first, second) in enumerate(cases):

        @pl.when(case == number)
        def _(first=first, second=second):
            for i in range(CHUNKS):
                fetch(arrays[first], low, 1, i).start()
                fetch(arrays[second], high, 2, i).start()

    @pl.when(case == len(cases))
    def _():
        for i in range(CHUNKS):
            fetch(head_ref, low, 1, i).start()
            fetch(head_ref, high, 2, i).start()

    def store(i):
        return pltpu.make_async_copy(
            result.at[parts[i]], o_ref.at[last, parts[i]], out_sems.at[i]
        )

    for i in range(CHUNKS):
        fetch(head_ref, own, 0, i).wait()
        fetch(head_ref, low, 1, i).wait()
        fetch(head_ref, high, 2, i).wait()
        both = low[parts[i]] + high[parts[i]]
        result[parts[i]] = own[parts[i]] - 0.5 * jnp.where(case < len(cases), both, 0.0)
        store(i).start()
    for i in range(CHUNKS):
        store(i).wait()


def lift_last(output, head, case, arrays, cases):
    _, rows, columns = output.shape
    whole = pl.BlockSpec(memory_space=pl.ANY)
    plane = pltpu.VMEM((rows, columns), jnp.float32)
    return pl.pallas_call(
        lambda *refs: last_kernel(*refs, cases=cases),
        in_specs=[pl.BlockSpec(memory_space=pltpu.SMEM)] + [whole] * (2 + len(arrays)),
        out_specs=whole,
        out_shape=jax.ShapeDtypeStruct(output.shape, jnp.float32),
        scratch_shapes=[plane] * 4
        + [pltpu.SemaphoreType.DMA((3, CHUNKS)), pltpu.SemaphoreType.DMA((CHUNKS,))],
        input_output_aliases={1: 0},
        name="lift_last",
    )(case, output, head, *arrays)


def exchange_plan(size):
    plan = {}
    quarter = size // 4
    plan["l1"] = ("head", [(c - 1, c) for c in range(size)])
    middle = [stride for stride in strides_of(size) if 8 <= stride <= quarter]
    for stride in middle:
        children = range(stride, size, 2 * stride)
        plan[f"r{stride}"] = ("head", [(c + stride, c) for c in children])
    for stride in [4] + middle:
        children = range(stride, size, 2 * stride)
        plan[f"l{stride}"] = ("head", [(c - stride, c) for c in children])
    plan["r1"] = ("head", [(c + 1, c) for c in range(1, size, 2)])
    plan["q2"] = ("l1", [(c + 3, c) for c in range(2, size, 4)])
    plan["top"] = (f"r{quarter}", [(3 * quarter, 2 * quarter)])
    plan["q4"] = ("l4", [(c + 8, c) for c in range(4, size, 8)])
    plan["q1"] = ("l1", [(c - 1, c) for c in range(2, size, 4)])
    return plan


def parent_names(stride, size):
    if stride == 1:
        return "l1", "r1"
    if stride == 2:
        return "q1", "q2"
    if stride == 4:
        return "l4", "q4"
    if stride == size // 2:
        return "top", "top"
    return f"l{stride}", f"r{stride}"


def on_device(nodal_values):
    size = lax.axis_size("gx")
    coarse_index = jnp.mod(lax.axis_index("gx") - 1, size)
    head = lift_head(nodal_values)
    planes = {"head": head}
    for name, (payload, pairs) in exchange_plan(size).items():
        route = [((a + 1) % size, (b + 1) % size) for a, b in pairs]
        planes[name] = lax.ppermute(planes[payload], "gx", route)
    output = lift_local(nodal_values, head, planes["l1"])
    names = [name for name in planes if name != "head"]
    pairs_of = [parent_names(stride, size) for stride in strides_of(size)]
    cases = [(names.index(a), names.index(b)) for a, b in pairs_of]
    case = jnp.full((1,), len(cases), jnp.int32)
    for number, stride in enumerate(strides_of(size)):
        case = jnp.where(jnp.mod(coarse_index, 2 * stride) == stride, number, case)
    return lift_last(output, head, case, [planes[name] for name in names], cases)


def solution(mesh):
    spec = P("gx", None, None)
    return jax.shard_map(
        on_device, mesh=mesh, in_specs=(spec,), out_specs=spec, check_vma=False
    )
```
